32 devices in a mesh: gx: 4 (over y, core), gy: 4 (over z), gz: 2 (over x).
Axes of the slice: x: 2, y: 2, z: 4, core: 2. Of those that a mesh axis runs over, the one named last changes fastest.
Arguments:
- face_blocks: float32 [4, 4, 2, 6, 16384], P('gx', 'gy', 'gz'), may hold values from -6 to 6
- owner_rank: int32 [4, 4, 2, 6, 1], P('gx', 'gy', 'gz'), may hold values from 0 to 3; in each aligned block of 6 rows (0 to 5, 6 to 11, ..., all dimensions but the last counted through in order) at most 2 rows name the same one
- owner_tile: int32 [4, 4, 2, 6], P('gx', 'gy', 'gz'), may hold values from 0 to 31
- live_count: int32 [4, 4, 2], P('gx', 'gy', 'gz'), may hold values from 1 to 6, as said below
- right_side: float32 [64, 256, 256], P('gx', 'gy', 'gz'), may hold values from -8 to 8
- diagonal: float32 [64, 256, 256], P('gx', 'gy', 'gz'), may hold values from 0.05 to 1
Outputs:
- solution_field: float32 [64, 256, 256], P('gx', 'gy', 'gz')
- residual: float32 [64, 256, 256], P('gx', 'gy', 'gz')
The draws below stay inside these ranges and needn't reach their ends.
Inputs may be any that keep to these rules, and one draw needn't show every extreme that they name: `owner_rank`: on one device no owner is named by more than 2 of the 6 slots, live or not; some owner is named exactly 2 times on some devices. `live_count`: some device has all 6 slots live in every draw.
All inputs are finite; a program needn't handle non-finite values.
Results may differ from the reference program's by a relative error of at most 0.00012.
Values sent between devices are 32-bit elements; how exact they have to be, the bound alone decides.
No kernel may reach another device: no remote copies, remote signals or barrier semaphores. Data moves between devices by JAX's collectives and lax.ppermute only.
A program may use at most 64 MiB of HBM per device.

```python
import math
import jax
import jax.numpy as jnp
import numpy as np

BLK = 128
CAP = 2
ITERS = 2
CX = 16
NB = 6
NX = 64
NY = 256
NZ = 256
N_GX = 4
N_GY = 4
N_GZ = 2


def draw_live_count(key, part):
    counts = jax.random.randint(key, (N_GX, N_GY, N_GZ), 1, NB + 1)
    return counts.at[0, 0, 0].set(NB).astype(jnp.int32)


def set_ends(array, key, smallest, largest):
    place = [jax.random.randint(jax.random.fold_in(key, axis), (), 0, length) for axis, length in enumerate(array.shape)]
    main_axis = array.shape.index(max(array.shape))
    neighbour = place[:main_axis] + [(place[main_axis] + 1) % array.shape[main_axis]] + place[main_axis + 1:]
    return array.at[tuple(place)].set(smallest).at[tuple(neighbour)].set(largest)


def block_scale(rng, dims, split, low, top_value):
    gain = 1.0
    for axis_at, parts in split:
        heights = jax.random.uniform(jax.random.fold_in(jax.random.fold_in(rng, 6), axis_at), (parts,), jnp.float32, low / len(split), top_value / len(split))
        gain = gain * jnp.repeat(jnp.exp(heights), dims[axis_at] // parts).reshape((-1,) + (1,) * (len(dims) - 1 - axis_at))
    return gain


def deal_out(key, own, number, rows, count, top, bound, skew):
    sequence = jax.random.permutation(key, count)
    packed, ordinary = portions_of(count, rows * top, bound, skew, True), portions_of(count, rows * top, bound, skew, False)
    places = jnp.arange(count)

    def named(lengths, turn):
        used = int((lengths > 0).sum())
        fixed = max(1, used // 4)
        shifted = fixed + (places - fixed + turn * (used - fixed)) % max(1, count - fixed)
        return jnp.zeros((count,), jnp.int32).at[sequence[jnp.where(places < fixed, places, shifted)]].set(jnp.asarray(lengths, jnp.int32))

    lengths = jnp.where(number % 4 == 0, named(packed, number // 4), named(ordinary, number - number // 4 - 1))
    mixed = jax.random.permutation(jax.random.fold_in(own, 3), count)
    donor, sink = mixed[0:count // 2 * 2:2], mixed[1:count // 2 * 2:2]
    margin = jnp.minimum(lengths[donor] - 1, bound - lengths[sink]) // 2
    margin = jnp.where((donor == sequence[0]) | (sink == sequence[0]) | (lengths[sink] == 0), 0, jnp.maximum(margin, 0))
    shifted = jax.random.randint(jax.random.fold_in(own, 4), (count // 2,), 0, 1 << 20) % (margin + 1)
    lengths = lengths.at[donor].add(-shifted).at[sink].add(shifted)
    members = jnp.searchsorted(jnp.cumsum(lengths), jnp.arange(rows * top), side="right").astype(jnp.int32)
    listing = members.reshape(top, rows).T
    listing = listing[jax.random.permutation(jax.random.fold_in(own, 1), rows)]
    turn = jax.random.randint(jax.random.fold_in(own, 2), (rows, 1), 0, top)
    return jnp.take_along_axis(listing, (jnp.arange(top)[None, :] + turn) % top, axis=1)


def portions_of(number_of, total, limit, slope, full):
    portions = [(1 << 20) // math.isqrt(standing ** slope) + 1 for standing in range(1, number_of + 1)]
    largest = limit if full else min(limit, max(-(-total // number_of), total * portions[0] // sum(portions)))
    least = 1 if total - largest >= number_of - 1 else 0
    given, spare = [largest] + [least] * (number_of - 1), total - largest - least * (number_of - 1)
    while spare > 0:
        movable = [i for i in range(1, number_of) if given[i] < largest] or [i for i in range(1, number_of) if given[i] < limit]
        mass, left = sum([portions[i] for i in movable]), spare
        for i in movable:
            more = min(limit - given[i], max(1, left * portions[i] // mass), spare)
            given[i] = given[i] + more
            spare = spare - more
    return np.array(given)


def scatter_about(own_key, dims, deviation, reach, split=(), held_as=jnp.bfloat16):
    values = jax.random.normal(own_key, dims, jnp.float32) * deviation
    if len(split) > 0:
        values = block_scale(own_key, dims, split, -0.22, 0.18) * values
    return jnp.clip(values, min=-reach, max=reach).astype(held_as)


def setup_inputs(seed: int = 0) -> dict:
    keys = jax.random.split(jax.random.key(seed), 7)
    face_blocks = scatter_about(keys[0], (N_GX, N_GY, N_GZ, NB, BLK * BLK), 1.0, 6.0, ((0, 4), (1, 4), (2, 2)), jnp.float32)
    owner_rank_keys = jax.random.split(jax.random.fold_in(keys[1], 1), N_GX * N_GY * N_GZ * NB // NB)
    owner_rank_turns = jax.random.permutation(jax.random.fold_in(keys[1], 3), N_GX * N_GY * N_GZ * NB // NB)
    owner_rank = jax.vmap(lambda own, number: deal_out(jax.random.fold_in(keys[1], 2), own, number, NB, N_GX, 1, CAP, 2))(owner_rank_keys, owner_rank_turns).reshape((N_GX, N_GY, N_GZ, NB, 1))
    owner_tile = set_ends(jax.random.randint(keys[2], (N_GX, N_GY, N_GZ, NB), 0, 2 * CX), jax.random.fold_in(keys[2], 1), 0, (2 * CX) - 1).astype(jnp.int32)
    live_count = draw_live_count(jax.random.fold_in(keys[6], 71), 0)
    right_side = scatter_about(keys[4], (NX, NY, NZ), 1.0, 8.0, ((0, 4), (1, 4), (2, 2)), jnp.float32)
    diagonal = jnp.clip(jnp.exp(math.log(1.0) - 2.9957323 * jax.random.uniform(keys[5], (NX, NY, NZ), jnp.float32) ** block_scale(keys[5], (NX, NY, NZ), ((0, 4), (1, 4), (2, 2)), -0.2, 0.2)), 0.05, 1.0)
    return dict(face_blocks=face_blocks, owner_rank=owner_rank, owner_tile=owner_tile, live_count=live_count, right_side=right_side, diagonal=diagonal)


def restrict(values):
    half = BLK // 2
    shaped = values.reshape(values.shape[:-1] + (half, 2, half, 2))
    summed = 0.25 * jnp.sum(shaped, axis=(-3, -1))
    return summed.reshape(values.shape[:-1] + (half * half,))


def operate(field, diagonal):
    padded = jnp.pad(field, 1)
    beside = padded[2:, 1:-1, 1:-1] + padded[:-2, 1:-1, 1:-1]
    beside = beside + padded[1:-1, 2:, 1:-1] + padded[1:-1, :-2, 1:-1]
    beside = beside + padded[1:-1, 1:-1, 2:] + padded[1:-1, 1:-1, :-2]
    return (6.0 + diagonal) * field - beside


def reference(face_blocks, owner_rank, owner_tile, live_count, right_side, diagonal):
    half = BLK // 2
    restricted = restrict(face_blocks)
    slots = jnp.arange(NB, dtype=jnp.int32)
    living = (slots[None, None, None, :] < live_count[..., None]).astype(jnp.float32)
    restricted = restricted * living[..., None]
    row_y = jnp.broadcast_to(jnp.arange(N_GY, dtype=jnp.int32)[None, :, None, None], (N_GX, N_GY, N_GZ, NB))
    row_z = jnp.broadcast_to(jnp.arange(N_GZ, dtype=jnp.int32)[None, None, :, None], (N_GX, N_GY, N_GZ, NB))
    target = owner_rank[..., 0].astype(jnp.int32)
    gathered = jnp.zeros((N_GX, N_GY, N_GZ, 2 * CX, half * half), jnp.float32)
    gathered = gathered.at[target, row_y, row_z, owner_tile.astype(jnp.int32)].add(restricted)
    shaped = gathered.reshape(N_GX, N_GY, N_GZ, CX, 2, half, half)
    source = jnp.transpose(shaped, (0, 3, 1, 5, 2, 4, 6)).reshape(NX, NY, NZ)
    load = right_side + source
    solution_field = jnp.zeros_like(load)
    residual, direction = load, load
    norm_now = jnp.sum(residual * residual)
    for iteration in range(ITERS):
        image = operate(direction, diagonal)
        alpha = norm_now / jnp.sum(direction * image)
        solution_field = solution_field + alpha * direction
        residual = residual - alpha * image
        norm_next = jnp.sum(residual * residual)
        direction = residual + (norm_next / norm_now) * direction
        norm_now = norm_next
    return solution_field, residual
```

```python
import functools

import jax
import jax.numpy as jnp
from jax import lax
from jax.experimental import pallas as pl
from jax.experimental.pallas import tpu as pltpu
from jax.sharding import PartitionSpec as P

CAP = 2
AXES = ("gx", "gy", "gz")
TAGS = 8
F32 = jnp.float32
VMEM = pl.BlockSpec(memory_space=pltpu.VMEM)
SMEM = pl.BlockSpec(memory_space=pltpu.SMEM)
S0, S1, V0, V1, V2, U0, U1, U2, E0, E1, SIG = range(11)
CORNER = 16
PAIRS = [(dx, dy, 0) for dx in (-1, 1) for dy in (-1, 1)]
PAIRS += [(dx, 0, dz) for dx in (-1, 1) for dz in (-1, 1)]
PAIRS += [(0, dy, dz) for dy in (-1, 1) for dz in (-1, 1)]


def params(mib=8):
    return pltpu.CompilerParams(vmem_limit_bytes=mib * 1024 * 1024)


def matchings(n):
    first = [(i, i ^ 1) for i in range(n) if (i ^ 1) < n]
    second = [(i, ((i + 1) ^ 1) - 1) for i in range(n) if 0 <= ((i + 1) ^ 1) - 1 < n]
    return [m for m in (first, second) if m]


def peer(i, k, n):
    return i ^ k if n & (n - 1) == 0 else (i + k) % n


def relative(owner, me, n):
    return owner ^ me if n & (n - 1) == 0 else lax.rem(owner - me + n, n)


def iotas(rows, lanes=128):
    shape = (rows, lanes)
    return lax.broadcasted_iota(jnp.int32, shape, 0), lax.broadcasted_iota(jnp.int32, shape, 1)


def roll(x, shift, axis):
    shift = shift % x.shape[axis]
    return x if shift == 0 else pltpu.roll(x, shift, axis)


def total(x):
    return jnp.sum(jnp.sum(x, axis=0, keepdims=True), axis=1, keepdims=True)


def fold(x):
    parts = [x[i : i + 8] for i in range(0, x.shape[0], 8)]
    while len(parts) > 1:
        rest = parts[len(parts) // 2 * 2 :]
        parts = [parts[i] + parts[i + 1] for i in range(0, len(parts) - 1, 2)] + rest
    return parts[0]


def flags(axis, n):
    at = lax.axis_index(axis)
    odd = lax.rem(at, 2) == 1
    low = jnp.where(at > 0, 1.0, 0.0).astype(F32)
    high = jnp.where(at < n - 1, 1.0, 0.0).astype(F32)
    return odd, low, high


def pick(odd, first, second):
    if second is None:
        return first, first
    return jnp.where(odd, first, second), jnp.where(odd, second, first)


def pack_kernel(n, owner_ref, tile_ref, live_ref, blocks_ref, out_ref):
    count, side = blocks_ref.shape[0], blocks_ref.shape[1]
    half = side // 2
    me = lax.axis_index("gx")
    live = live_ref[0]
    src, dst = iotas(side, side)
    gather = jnp.where(src // 2 == dst % half, 0.25, 0.0).astype(jnp.bfloat16)
    out_ref[...] = jnp.zeros_like(out_ref)
    _, lane = iotas(half)
    _, lane_t = iotas(TAGS)
    for i in range(count):
        rows = blocks_ref[i, pl.ds(0, half, 2), :] + blocks_ref[i, pl.ds(1, half, 2), :]
        a = rows.astype(jnp.bfloat16)
        rest = rows - a.astype(F32)
        b = rest.astype(jnp.bfloat16)
        c = (rest - b.astype(F32)).astype(jnp.bfloat16)
        both = sum(jnp.dot(p, gather, preferred_element_type=F32) for p in (c, b, a))
        owner = owner_ref[i]
        slot = jnp.int32(0)
        for j in range(i):
            slot = slot + jnp.where(owner_ref[j] == owner, 1, 0)
        tag = jnp.where(i < live, tile_ref[i] + 1, 0).astype(F32)
        to = relative(owner, me, n)
        old = out_ref[pl.ds(to, 1), 0:half, :][0]
        new = jnp.where(lane // half == slot, both, old)
        out_ref[pl.ds(to, 1), 0:half, :] = new[None]
        old = out_ref[pl.ds(to, 1), half : half + TAGS, :][0]
        new = jnp.where(lane_t // half == slot, tag, old)
        out_ref[pl.ds(to, 1), half : half + TAGS, :] = new[None]


def local_operator(layer, x, count, here, diag, row, lane):
    rows = here.shape[0]
    beside = jnp.where(row == 0, 0.0, roll(here, 1, 0)) + jnp.where(
        row == rows - 1, 0.0, roll(here, -1, 0)
    )
    beside = beside + jnp.where(lane == 0, 0.0, roll(here, 1, 1))
    beside = beside + jnp.where(lane == 127, 0.0, roll(here, -1, 1))
    if x > 0:
        beside = beside + layer(x - 1)
    if x < count - 1:
        beside = beside + layer(x + 1)
    return (6.0 + diag) * here - beside


def load_kernel(sizes, dims, *refs):
    nx, ny, nz = sizes
    X, Y = dims
    chunks, (rhs_ref, diag_ref), rest = refs[:nx], refs[nx : nx + 2], refs[nx + 2 :]
    r_ref, pw_ref = rest[:2]
    face_refs, turned = rest[2:-1], rest[-1]
    row, lane = iotas(Y)
    half = Y
    _, lane1 = iotas(1)
    tags = []
    for k, ref in enumerate(chunks):
        turned[k * Y : (k + 1) * Y, :] = roll(ref[0:half, :], half, 1)
        tag = ref[half : half + 1, :]
        tags.append((tag, roll(tag, half, 1)))
    for x in range(X):
        want = (2 * x + 1 + lane1 // half).astype(F32)
        acc = rhs_ref[x * Y : (x + 1) * Y, :]
        for k, ref in enumerate(chunks):
            straight, swapped = tags[k]
            acc = acc + jnp.where(straight == want, ref[0:half, :], 0.0)
            acc = acc + jnp.where(swapped == want, turned[k * Y : (k + 1) * Y, :], 0.0)
        r_ref[x * Y : (x + 1) * Y, :] = acc

    def layer(x):
        return r_ref[x * Y : (x + 1) * Y, :]

    tile = jnp.zeros((Y, 128), F32)
    for x in range(X):
        here = layer(x)
        pw = local_operator(layer, x, X, here, diag_ref[x * Y : (x + 1) * Y, :], row, lane)
        pw_ref[x * Y : (x + 1) * Y, :] = pw
        tile = jnp.where(lane // 2 == x, roll(here, 2 * x + 1, 1), tile)
        tile = jnp.where(lane // 2 == X + x, roll(pw, 2 * (X + x) + 1, 1), tile)
    faces = iter(face_refs)
    odd, _, _ = flags("gx", nx)
    for m in range(len(matchings(nx))):
        top = jnp.where(odd, 0, (X - 1) * Y) if m == 0 else jnp.where(odd, (X - 1) * Y, 0)
        top = pl.multiple_of(top, Y)
        out = next(faces)
        out[0:Y, :] = r_ref[pl.ds(top, Y), :]
        out[Y : 2 * Y, :] = pw_ref[pl.ds(top, Y), :]
    odd, _, _ = flags("gy", ny)
    for m in range(len(matchings(ny))):
        out = next(faces)
        for j, ref in enumerate((r_ref, pw_ref)):
            low, high = ref[pl.ds(0, X, Y), :], ref[pl.ds(Y - 1, X, Y), :]
            out[j * X : (j + 1) * X, :] = jnp.where(odd, low, high) if m == 0 else jnp.where(
                odd, high, low
            )
    next(faces)[...] = tile


def moment_kernel(sizes, dims, *refs):
    nx, ny, nz = sizes
    X, Y = dims
    refs = list(refs)
    r_ref, pw_ref, diag_ref, tile_ref = refs[:4]
    refs = refs[4:]

    def received(n):
        got = [refs.pop(0) for _ in matchings(n)]
        return got + [None] * (2 - len(got))

    fx, fy, fz = received(nx), received(ny), received(nz)
    w_ref, s_ref, pay_ref, hw_ref = refs
    row, lane = iotas(Y)
    _, lane1 = iotas(1)

    def faces(got, axis, n, a, b):
        odd, low, high = flags(axis, n)
        if not [g for g in got if g is not None]:
            return jnp.zeros((b - a, 128), F32), jnp.zeros((b - a, 128), F32), low, high
        one, two = [None if g is None else g[a:b, :] for g in got]
        lo, hi = pick(odd, one, two)
        return lo * low, hi * high, low, high

    xlr, xhr, x_low, x_high = faces(fx, "gx", nx, 0, Y)
    xlp, xhp, _, _ = faces(fx, "gx", nx, Y, 2 * Y)
    ylr, yhr, y_low, y_high = faces(fy, "gy", ny, 0, X)
    ylp, yhp, _, _ = faces(fy, "gy", ny, X, 2 * X)
    zl, zh, z_low, z_high = faces(fz, "gz", nz, 0, Y)
    zt = jnp.where(lane % 2 == 0, roll(zh, -1, 1), roll(zl, 1, 1))
    zflag = jnp.where(lane1 == 0, z_low, jnp.where(lane1 == 127, z_high, 0.0))

    acc = {k: jnp.zeros((8, 128), F32) for k in (S0, S1, V0, V1, V2, U0, U1, U2, E0, E1)}

    def add(key, value):
        acc[key] = acc[key] + fold(value)

    for x in range(X):
        zr_all = roll(zt, -(2 * x + 1), 1)
        zp_all = roll(zt, -(2 * (X + x) + 1), 1)
        for lo, hi in ((0, 8), (8, Y - 8), (Y - 8, Y)):
            sl = slice(x * Y + lo, x * Y + hi)
            r, pw = r_ref[sl, :], pw_ref[sl, :]
            on_z = jnp.where((lane == 0) | (lane == 127), zflag, 0.0)[lo:hi]
            zr = jnp.where(on_z > 0.0, zr_all[lo:hi], 0.0)
            zw = jnp.where(on_z > 0.0, zp_all[lo:hi] - r, 0.0)
            hr, hw, hp, h2, n = zr, zw, zw * zr, zr * zr, on_z
            edge = False
            if lo == 0 or hi == Y:
                edge = True
                at = row[lo:hi] == (0 if lo == 0 else Y - 1)
                fr, fp, flag = (ylr, ylp, y_low) if lo == 0 else (yhr, yhp, y_high)
                yr = jnp.where(at, fr[x : x + 1], 0.0)
                yw = jnp.where(at, (fp[x : x + 1] - r) * flag, 0.0)
                hr, hw, hp, h2 = hr + yr, hw + yw, hp + yw * yr, h2 + yr * yr
                n = n + jnp.where(at, flag, 0.0)
            for end, fr, fp, flag in ((0, xlr, xlp, x_low), (X - 1, xhr, xhp, x_high)):
                if x == end:
                    edge = True
                    xr = fr[lo:hi]
                    xw = (fp[lo:hi] - r) * flag
                    hr, hw, hp, h2 = hr + xr, hw + xw, hp + xw * xr, h2 + xr * xr
                    n = n + flag
            w = pw - hr
            w_ref[sl, :] = w
            hw_ref[sl, :] = hw
            add(S0, r * r)
            add(S1, r * w)
            if edge:
                add(E0, hr * hr - h2)
                add(E1, hw * hr - hp - (n - 1.0) * r * hr)

    s0, s1 = total(acc[S0]), total(acc[S1])
    sigma = jnp.where(s1 > 0.0, s0 / jnp.where(s1 > 0.0, s1, 1.0), 0.15)
    sigma = jnp.clip(sigma, 0.05, 20.0)

    def layer(x):
        return w_ref[x * Y : (x + 1) * Y, :]

    for x in range(X):
        sl = slice(x * Y, (x + 1) * Y)
        w, r = layer(x), r_ref[sl, :]
        s = local_operator(layer, x, X, w, diag_ref[sl, :], row, lane) - hw_ref[sl, :]
        s_ref[sl, :] = s
        sw = sigma * w
        v = r - sw
        u = w - sigma * s
        add(V0, v * v)
        add(V1, v * w)
        add(V2, w * w)
        add(U0, v * u)
        add(U1, (v - sw) * s + w * w)
        add(U2, w * s)

    mom = jnp.where(lane1 == SIG, sigma, 0.0)
    for k, part in acc.items():
        value = s0 if k == S0 else s1 if k == S1 else total(part)
        mom = jnp.where(lane1 == k, value, mom)
    for j in range(4):
        at = (X - 1 if j // 2 else 0) * Y + (Y - 1 if j % 2 else 0)
        mom = jnp.where(lane1 // 2 == CORNER // 2 + j, roll(r_ref[at : at + 1, :], CORNER + 2 * j + 1, 1), mom)
    count = pay_ref.shape[0]
    parity, _ = iotas(count)
    pay_ref[...] = jnp.where(parity % 2 == 0, mom, 0.0)
    tile = tile_ref[...]
    for dx, dy, dz in PAIRS:
        exists, to = neighbour(sizes, dx, dy, dz)
        x, y = (X - 1 if dx > 0 else 0), (Y - 1 if dy > 0 else 0)
        if dz == 0:
            line = r_ref[x * Y + y : x * Y + y + 1, :]
        elif dx == 0:
            line = tile_ref[y : y + 1, :]
        else:
            column = jnp.sum(jnp.where(lane == 2 * x + (0 if dz > 0 else 1), tile, 0.0), axis=1, keepdims=True)
            line = jnp.sum(jnp.where(row == lane, column, 0.0), axis=0, keepdims=True)
        pay_ref[pl.ds(2 * to + 1, 1), :] = line


def neighbour(sizes, dx, dy, dz):
    at = [lax.axis_index(a) for a in AXES]
    to = [p + d for p, d in zip(at, (dx, dy, dz))]
    good = None
    for p, n in zip(to, sizes):
        ok = (p >= 0) & (p < n)
        good = ok if good is None else good & ok
    flat = (to[0] * sizes[1] + to[1]) * sizes[2] + to[2]
    own = (at[0] * sizes[1] + at[1]) * sizes[2] + at[2]
    return jnp.where(good, 1.0, 0.0).astype(F32), jnp.where(good, flat, own)


def final_kernel(sizes, dims, pay_ref, r_ref, w_ref, s_ref, x_out, r_out):
    nx, ny, nz = sizes
    X, Y = dims
    devices = nx * ny * nz
    row, lane = iotas(Y)
    _, lane1 = iotas(1)
    drow, dlane = iotas(devices)
    mom = pay_ref[pl.ds(0, devices, 2), :]

    def column(k):
        return jnp.sum(jnp.where(dlane == k, mom, 0.0), axis=1, keepdims=True)

    def over(x):
        return jnp.sum(x, axis=0, keepdims=True)

    sums = over(mom)

    def lane_of(k):
        return jnp.sum(jnp.where(lane1 == k, sums, 0.0), axis=1, keepdims=True)

    norm0, rw = lane_of(S0), lane_of(S1)
    alpha = norm0 / rw
    delta = column(SIG) - alpha
    v1, v2 = column(V1), column(V2)
    norm1 = over(column(V0) + delta * (2.0 * v1 + delta * v2))
    r1w = over(v1 + delta * v2)
    r1ar1 = over(column(U0) + delta * (column(U1) + delta * column(U2)))
    place = [drow // (ny * nz), (drow // nz) % ny, drow % nz]
    opposite = jnp.zeros((devices, 128), F32)
    for dy in (-1, 1):
        for dz in (-1, 1):
            mine = CORNER + 2 * (2 + (dy > 0)) + (0 if dz > 0 else 1)
            theirs = CORNER + 2 * (0 + (dy < 0)) + (1 if dz > 0 else 0)
            step = (ny + dy) * nz + dz
            ok = (place[0] < nx - 1) & (place[1] + dy >= 0) & (place[1] + dy < ny)
            ok = ok & (place[2] + dz >= 0) & (place[2] + dz < nz) & (dlane == mine)
            other = roll(roll(mom, -step, 0), mine - theirs, 1)
            opposite = opposite + jnp.where(ok, mom * other, 0.0)
    e1 = lane_of(E1) - 12.0 * total(opposite)
    r1ar1 = r1ar1 - alpha * lane_of(E0) + alpha * alpha * e1
    beta = norm1 / norm0
    alpha1 = norm1 / (r1ar1 + beta * (2.0 * r1w + beta * rw))

    xy, xz, yz = {}, {}, {}
    for dx, dy, dz in PAIRS:
        exists, at = neighbour(sizes, dx, dy, dz)
        line = pay_ref[pl.ds(2 * at + 1, 1), :] * (2.0 * exists)
        if dz == 0:
            xy[dx, dy] = line
        elif dx == 0:
            yz[dy, dz] = line
        else:
            xz[dx, dz] = jnp.sum(jnp.where(row == lane, line, 0.0), axis=1, keepdims=True)
    row8, lane8 = iotas(8)
    rim = {}
    for dy in (-1, 1):
        rim[dy] = jnp.where(lane1 % 2 == 0, roll(yz[dy, 1], -1, 1), roll(yz[dy, -1], 1, 1))
    rim = jnp.where(row8 == 0, rim[-1], jnp.where(row8 == 7, rim[1], 0.0))
    sides = (lane8 == 0) | (lane8 == 127)

    for x in range(X):
        turned = jnp.where(sides, roll(rim, -(2 * x + 1), 1), 0.0)
        for lo, hi in ((0, 8), (8, Y - 8), (Y - 8, Y)):
            sl = slice(x * Y + lo, x * Y + hi)
            r, w, s = r_ref[sl, :], w_ref[sl, :], s_ref[sl, :]
            dx = -1 if x == 0 else 1 if x == X - 1 else 0
            dy = -1 if lo == 0 else 1 if hi == Y else 0
            if dy:
                at = row8 == (0 if dy < 0 else 7)
                s = s + jnp.where(at, turned, 0.0)
                if dx:
                    s = s + jnp.where(at, xy[dx, dy], 0.0)
            if dx:
                ln = lane[lo:hi]
                s = s + jnp.where(ln == 0, xz[dx, -1][lo:hi], jnp.where(ln == 127, xz[dx, 1][lo:hi], 0.0))
            r1 = r - alpha * w
            x_out[sl, :] = alpha * r + alpha1 * (r1 + beta * r)
            r_out[sl, :] = r1 - alpha1 * (w - alpha * s + beta * w)


def per_device(face_blocks, owner_rank, owner_tile, live_count, right_side, diagonal):
    sizes = tuple(lax.axis_size(a) for a in AXES)
    nx, ny, nz = sizes
    X, Y, Z = right_side.shape
    dims = (X, Y)
    count = face_blocks.shape[3]
    side = 2 * Y
    flat = jax.ShapeDtypeStruct((X * Y, Z), F32)
    rhs, diag = right_side.reshape(X * Y, Z), diagonal.reshape(X * Y, Z)

    packed = pl.pallas_call(
        functools.partial(pack_kernel, nx),
        out_shape=jax.ShapeDtypeStruct((nx, Y + TAGS, 128), F32),
        in_specs=[SMEM, SMEM, SMEM, VMEM],
        out_specs=VMEM,
        compiler_params=params(),
        name="pack",
    )(
        owner_rank.reshape(count),
        owner_tile.reshape(count),
        live_count.reshape(1),
        face_blocks.reshape(count, side, side),
    )
    chunks = [packed[0]]
    for k in range(1, nx):
        chunks.append(lax.ppermute(packed[k], "gx", [(i, peer(i, k, nx)) for i in range(nx)]))

    def face_shapes():
        shapes = [(2 * Y, Z)] * len(matchings(nx)) + [(2 * X, Z)] * len(matchings(ny)) + [(Y, Z)]
        return [jax.ShapeDtypeStruct(s, F32) for s in shapes]

    r, pw, *faces = pl.pallas_call(
        functools.partial(load_kernel, sizes, dims),
        out_shape=[flat, flat] + face_shapes(),
        in_specs=[VMEM] * (nx + 2),
        out_specs=[VMEM] * (2 + len(face_shapes())),
        scratch_shapes=[pltpu.VMEM((nx * Y, 128), F32)],
        compiler_params=params(),
        name="load",
    )(*chunks, rhs, diag)
    tile = faces[-1]
    got = []
    sent = iter(faces[:-1])
    for axis, n in (("gx", nx), ("gy", ny)):
        for pairs in matchings(n):
            got.append(lax.ppermute(next(sent), axis, pairs))
    for pairs in matchings(nz):
        got.append(lax.ppermute(tile, "gz", pairs))

    w, s, pay = pl.pallas_call(
        functools.partial(moment_kernel, sizes, dims),
        out_shape=[flat, flat, jax.ShapeDtypeStruct((2 * nx * ny * nz, 128), F32)],
        in_specs=[VMEM] * (4 + len(got)),
        out_specs=[VMEM] * 3,
        scratch_shapes=[pltpu.VMEM((X * Y, 128), F32)],
        compiler_params=params(),
        name="moments",
    )(r, pw, diag, tile, *got)
    pay = lax.all_to_all(pay, AXES, split_axis=0, concat_axis=0, tiled=True)
    x2, r2 = pl.pallas_call(
        functools.partial(final_kernel, sizes, dims),
        out_shape=[flat, flat],
        in_specs=[VMEM] * 4,
        out_specs=[VMEM] * 2,
        compiler_params=params(),
        name="final",
    )(pay, r, w, s)
    return x2.reshape(X, Y, Z), r2.reshape(X, Y, Z)


def solution(mesh):
    return jax.shard_map(
        per_device,
        mesh=mesh,
        in_specs=(
            P("gx", "gy", "gz", None, None),
            P("gx", "gy", "gz", None, None),
            P("gx", "gy", "gz", None),
            P("gx", "gy", "gz"),
            P("gx", "gy", "gz"),
            P("gx", "gy", "gz"),
        ),
        out_specs=(P("gx", "gy", "gz"), P("gx", "gy", "gz")),
        check_vma=False,
    )
```

```python
import functools

import jax
import jax.numpy as jnp
from jax import lax
from jax.experimental import pallas as pl
from jax.experimental.pallas import tpu as pltpu
from jax.sharding import PartitionSpec as P

AXES = ("gx", "gy", "gz")
TAGS = 8
F32 = jnp.float32
VMEM = pl.BlockSpec(memory_space=pltpu.VMEM)
HBM = pl.BlockSpec(memory_space=pltpu.HBM)
S0, S1, V0, V1, V2, U0, U1, U2, E0, E1, SIG = range(11)
CORNER = 16
PAIRS = [(dx, dy, 0) for dx in (-1, 1) for dy in (-1, 1)]
PAIRS += [(dx, 0, dz) for dx in (-1, 1) for dz in (-1, 1)]
PAIRS += [(0, dy, dz) for dy in (-1, 1) for dz in (-1, 1)]


def params(mib=8):
    return pltpu.CompilerParams(vmem_limit_bytes=mib * 1024 * 1024)


def in_hbm(x):
    return pltpu.with_memory_space_constraint(x, pltpu.HBM)


def matchings(n):
    first = [(i, i ^ 1) for i in range(n) if (i ^ 1) < n]
    second = [(i, ((i + 1) ^ 1) - 1) for i in range(n) if 0 <= ((i + 1) ^ 1) - 1 < n]
    return [m for m in (first, second) if m]


def peer(i, k, n):
    return i ^ k if n & (n - 1) == 0 else (i + k) % n


def relative(owner, me, n):
    return owner ^ me if n & (n - 1) == 0 else lax.rem(owner - me + n, n)


def iotas(rows, lanes=128):
    shape = (rows, lanes)
    return lax.broadcasted_iota(jnp.int32, shape, 0), lax.broadcasted_iota(jnp.int32, shape, 1)


def roll(x, shift, axis):
    shift = shift % x.shape[axis]
    return x if shift == 0 else pltpu.roll(x, shift, axis)


def total(x):
    return jnp.sum(jnp.sum(x, axis=0, keepdims=True), axis=1, keepdims=True)


def fold(x):
    parts = [x[i : i + 8] for i in range(0, x.shape[0], 8)]
    while len(parts) > 1:
        rest = parts[len(parts) // 2 * 2 :]
        parts = [parts[i] + parts[i + 1] for i in range(0, len(parts) - 1, 2)] + rest
    return parts[0]


def flags(axis, n):
    at = lax.axis_index(axis)
    odd = lax.rem(at, 2) == 1
    low = jnp.where(at > 0, 1.0, 0.0).astype(F32)
    high = jnp.where(at < n - 1, 1.0, 0.0).astype(F32)
    return odd, low, high


def pick(odd, first, second):
    if second is None:
        return first, first
    return jnp.where(odd, first, second), jnp.where(odd, second, first)


def pack_kernel(
    n, owner_hbm, tile_hbm, live_hbm, blocks_hbm, rhs_hbm, diag_hbm,
    out_ref, rhs_ref, diag_ref,
    owner_ref, tile_ref, live_ref, blocks_ref, small_sem, block_sem, field_sem,
):
    count, side = blocks_ref.shape[0], blocks_ref.shape[1]
    half = side // 2
    small = [
        pltpu.make_async_copy(a, b, small_sem.at[i])
        for i, (a, b) in enumerate(
            ((owner_hbm, owner_ref), (tile_hbm, tile_ref), (live_hbm, live_ref))
        )
    ]
    blocks = [
        pltpu.make_async_copy(blocks_hbm.at[i], blocks_ref.at[i], block_sem.at[i])
        for i in range(count)
    ]
    fields = [
        pltpu.make_async_copy(rhs_hbm, rhs_ref, field_sem.at[0]),
        pltpu.make_async_copy(diag_hbm, diag_ref, field_sem.at[1]),
    ]
    for copy in small + blocks + fields:
        copy.start()
    me = lax.axis_index("gx")
    src, dst = iotas(side, side)
    gather = jnp.where(src // 2 == dst % half, 0.25, 0.0).astype(jnp.bfloat16)
    out_ref[...] = jnp.zeros_like(out_ref)
    _, lane = iotas(half)
    _, lane_t = iotas(TAGS)
    for copy in small:
        copy.wait()
    live = live_ref[0]
    for i in range(count):
        blocks[i].wait()
        rows = blocks_ref[i, pl.ds(0, half, 2), :] + blocks_ref[i, pl.ds(1, half, 2), :]
        a = rows.astype(jnp.bfloat16)
        rest = rows - a.astype(F32)
        b = rest.astype(jnp.bfloat16)
        c = (rest - b.astype(F32)).astype(jnp.bfloat16)
        both = sum(jnp.dot(p, gather, preferred_element_type=F32) for p in (c, b, a))
        owner = owner_ref[i]
        slot = jnp.int32(0)
        for j in range(i):
            slot = slot + jnp.where(owner_ref[j] == owner, 1, 0)
        tag = jnp.where(i < live, tile_ref[i] + 1, 0).astype(F32)
        to = relative(owner, me, n)
        old = out_ref[pl.ds(to, 1), 0:half, :][0]
        new = jnp.where(lane // half == slot, both, old)
        out_ref[pl.ds(to, 1), 0:half, :] = new[None]
        old = out_ref[pl.ds(to, 1), half : half + TAGS, :][0]
        new = jnp.where(lane_t // half == slot, tag, old)
        out_ref[pl.ds(to, 1), half : half + TAGS, :] = new[None]
    for copy in fields:
        copy.wait()


def local_operator(layer, x, count, here, diag, row, lane):
    rows = here.shape[0]
    beside = jnp.where(row == 0, 0.0, roll(here, 1, 0)) + jnp.where(
        row == rows - 1, 0.0, roll(here, -1, 0)
    )
    beside = beside + jnp.where(lane == 0, 0.0, roll(here, 1, 1))
    beside = beside + jnp.where(lane == 127, 0.0, roll(here, -1, 1))
    if x > 0:
        beside = beside + layer(x - 1)
    if x < count - 1:
        beside = beside + layer(x + 1)
    return (6.0 + diag) * here - beside


def load_kernel(sizes, dims, *refs):
    nx, ny, _ = sizes
    X, Y = dims
    chunks, (rhs_ref, diag_ref), rest = refs[:nx], refs[nx : nx + 2], refs[nx + 2 :]
    r_ref, pw_ref = rest[:2]
    face_refs, turned = rest[2:-1], rest[-1]
    row, lane = iotas(Y)
    half = Y
    _, lane1 = iotas(1)
    tags = []
    for k, ref in enumerate(chunks):
        turned[k * Y : (k + 1) * Y, :] = roll(ref[0:half, :], half, 1)
        tag = ref[half : half + 1, :]
        tags.append((tag, roll(tag, half, 1)))
    for x in range(X):
        want = (2 * x + 1 + lane1 // half).astype(F32)
        acc = rhs_ref[x * Y : (x + 1) * Y, :]
        for k, ref in enumerate(chunks):
            straight, swapped = tags[k]
            acc = acc + jnp.where(straight == want, ref[0:half, :], 0.0)
            acc = acc + jnp.where(swapped == want, turned[k * Y : (k + 1) * Y, :], 0.0)
        r_ref[x * Y : (x + 1) * Y, :] = acc

    def layer(x):
        return r_ref[x * Y : (x + 1) * Y, :]

    tile = jnp.zeros((Y, 128), F32)
    for x in range(X):
        here = layer(x)
        pw = local_operator(layer, x, X, here, diag_ref[x * Y : (x + 1) * Y, :], row, lane)
        pw_ref[x * Y : (x + 1) * Y, :] = pw
        tile = jnp.where(lane // 2 == x, roll(here, 2 * x + 1, 1), tile)
        tile = jnp.where(lane // 2 == X + x, roll(pw, 2 * (X + x) + 1, 1), tile)
    faces = iter(face_refs)
    odd, _, _ = flags("gx", nx)
    for m in range(len(matchings(nx))):
        top = jnp.where(odd, 0, (X - 1) * Y) if m == 0 else jnp.where(odd, (X - 1) * Y, 0)
        top = pl.multiple_of(top, Y)
        out = next(faces)
        out[0:Y, :] = r_ref[pl.ds(top, Y), :]
        out[Y : 2 * Y, :] = pw_ref[pl.ds(top, Y), :]
    odd, _, _ = flags("gy", ny)
    for m in range(len(matchings(ny))):
        out = next(faces)
        for j, ref in enumerate((r_ref, pw_ref)):
            low, high = ref[pl.ds(0, X, Y), :], ref[pl.ds(Y - 1, X, Y), :]
            out[j * X : (j + 1) * X, :] = jnp.where(odd, low, high) if m == 0 else jnp.where(
                odd, high, low
            )
    next(faces)[...] = tile


def moment_kernel(sizes, dims, *refs):
    nx, ny, nz = sizes
    X, Y = dims
    refs = list(refs)
    r_ref, pw_ref, diag_ref, tile_ref = refs[:4]
    refs = refs[4:]

    def received(n):
        got = [refs.pop(0) for _ in matchings(n)]
        return got + [None] * (2 - len(got))

    fx, fy, fz = received(nx), received(ny), received(nz)
    w_ref, s_ref, pay_ref, hw_ref = refs
    row, lane = iotas(Y)
    _, lane1 = iotas(1)

    def faces(got, axis, n, a, b):
        odd, low, high = flags(axis, n)
        if not [g for g in got if g is not None]:
            return jnp.zeros((b - a, 128), F32), jnp.zeros((b - a, 128), F32), low, high
        one, two = [None if g is None else g[a:b, :] for g in got]
        lo, hi = pick(odd, one, two)
        return lo * low, hi * high, low, high

    xlr, xhr, x_low, x_high = faces(fx, "gx", nx, 0, Y)
    xlp, xhp, _, _ = faces(fx, "gx", nx, Y, 2 * Y)
    ylr, yhr, y_low, y_high = faces(fy, "gy", ny, 0, X)
    ylp, yhp, _, _ = faces(fy, "gy", ny, X, 2 * X)
    zl, zh, z_low, z_high = faces(fz, "gz", nz, 0, Y)
    zt = jnp.where(lane % 2 == 0, roll(zh, -1, 1), roll(zl, 1, 1))
    zflag = jnp.where(lane1 == 0, z_low, jnp.where(lane1 == 127, z_high, 0.0))

    acc = {k: jnp.zeros((8, 128), F32) for k in (S0, S1, V0, V1, V2, U0, U1, U2, E0, E1)}

    def add(key, value):
        acc[key] = acc[key] + fold(value)

    for x in range(X):
        zr_all = roll(zt, -(2 * x + 1), 1)
        zp_all = roll(zt, -(2 * (X + x) + 1), 1)
        for lo, hi in ((0, 8), (8, Y - 8), (Y - 8, Y)):
            sl = slice(x * Y + lo, x * Y + hi)
            r, pw = r_ref[sl, :], pw_ref[sl, :]
            on_z = jnp.where((lane == 0) | (lane == 127), zflag, 0.0)[lo:hi]
            zr = jnp.where(on_z > 0.0, zr_all[lo:hi], 0.0)
            zw = jnp.where(on_z > 0.0, zp_all[lo:hi] - r, 0.0)
            hr, hw, hp, h2, n = zr, zw, zw * zr, zr * zr, on_z
            edge = False
            if lo == 0 or hi == Y:
                edge = True
                at = row[lo:hi] == (0 if lo == 0 else Y - 1)
                fr, fp, flag = (ylr, ylp, y_low) if lo == 0 else (yhr, yhp, y_high)
                yr = jnp.where(at, fr[x : x + 1], 0.0)
                yw = jnp.where(at, (fp[x : x + 1] - r) * flag, 0.0)
                hr, hw, hp, h2 = hr + yr, hw + yw, hp + yw * yr, h2 + yr * yr
                n = n + jnp.where(at, flag, 0.0)
            for end, fr, fp, flag in ((0, xlr, xlp, x_low), (X - 1, xhr, xhp, x_high)):
                if x == end:
                    edge = True
                    xr = fr[lo:hi]
                    xw = (fp[lo:hi] - r) * flag
                    hr, hw, hp, h2 = hr + xr, hw + xw, hp + xw * xr, h2 + xr * xr
                    n = n + flag
            w = pw - hr
            w_ref[sl, :] = w
            hw_ref[sl, :] = hw
            add(S0, r * r)
            add(S1, r * w)
            if edge:
                add(E0, hr * hr - h2)
                add(E1, hw * hr - hp - (n - 1.0) * r * hr)

    s0, s1 = total(acc[S0]), total(acc[S1])
    sigma = jnp.where(s1 > 0.0, s0 / jnp.where(s1 > 0.0, s1, 1.0), 0.15)
    sigma = jnp.clip(sigma, 0.05, 20.0)

    def layer(x):
        return w_ref[x * Y : (x + 1) * Y, :]

    for x in range(X):
        sl = slice(x * Y, (x + 1) * Y)
        w, r = layer(x), r_ref[sl, :]
        s = local_operator(layer, x, X, w, diag_ref[sl, :], row, lane) - hw_ref[sl, :]
        s_ref[sl, :] = s
        sw = sigma * w
        v = r - sw
        u = w - sigma * s
        add(V0, v * v)
        add(V1, v * w)
        add(V2, w * w)
        add(U0, v * u)
        add(U1, (v - sw) * s + w * w)
        add(U2, w * s)

    mom = jnp.where(lane1 == SIG, sigma, 0.0)
    for k, part in acc.items():
        value = s0 if k == S0 else s1 if k == S1 else total(part)
        mom = jnp.where(lane1 == k, value, mom)
    for j in range(4):
        at = (X - 1 if j // 2 else 0) * Y + (Y - 1 if j % 2 else 0)
        mom = jnp.where(lane1 // 2 == CORNER // 2 + j, roll(r_ref[at : at + 1, :], CORNER + 2 * j + 1, 1), mom)
    count = pay_ref.shape[0]
    parity, _ = iotas(count)
    pay_ref[...] = jnp.where(parity % 2 == 0, mom, 0.0)
    tile = tile_ref[...]
    for dx, dy, dz in PAIRS:
        _, to = neighbour(sizes, dx, dy, dz)
        x, y = (X - 1 if dx > 0 else 0), (Y - 1 if dy > 0 else 0)
        if dz == 0:
            line = r_ref[x * Y + y : x * Y + y + 1, :]
        elif dx == 0:
            line = tile_ref[y : y + 1, :]
        else:
            column = jnp.sum(jnp.where(lane == 2 * x + (0 if dz > 0 else 1), tile, 0.0), axis=1, keepdims=True)
            line = jnp.sum(jnp.where(row == lane, column, 0.0), axis=0, keepdims=True)
        pay_ref[pl.ds(2 * to + 1, 1), :] = line


def neighbour(sizes, dx, dy, dz):
    at = [lax.axis_index(a) for a in AXES]
    to = [p + d for p, d in zip(at, (dx, dy, dz))]
    good = None
    for p, n in zip(to, sizes):
        ok = (p >= 0) & (p < n)
        good = ok if good is None else good & ok
    flat = (to[0] * sizes[1] + to[1]) * sizes[2] + to[2]
    own = (at[0] * sizes[1] + at[1]) * sizes[2] + at[2]
    return jnp.where(good, 1.0, 0.0).astype(F32), jnp.where(good, flat, own)


def final_kernel(sizes, dims, pay_ref, r_ref, w_ref, s_ref, x_out, r_out):
    nx, ny, nz = sizes
    X, Y = dims
    devices = nx * ny * nz
    row, lane = iotas(Y)
    _, lane1 = iotas(1)
    drow, dlane = iotas(devices)
    mom = pay_ref[pl.ds(0, devices, 2), :]

    def column(k):
        return jnp.sum(jnp.where(dlane == k, mom, 0.0), axis=1, keepdims=True)

    def over(x):
        return jnp.sum(x, axis=0, keepdims=True)

    sums = over(mom)

    def lane_of(k):
        return jnp.sum(jnp.where(lane1 == k, sums, 0.0), axis=1, keepdims=True)

    norm0, rw = lane_of(S0), lane_of(S1)
    alpha = norm0 / rw
    delta = column(SIG) - alpha
    v1, v2 = column(V1), column(V2)
    norm1 = over(column(V0) + delta * (2.0 * v1 + delta * v2))
    r1w = over(v1 + delta * v2)
    r1ar1 = over(column(U0) + delta * (column(U1) + delta * column(U2)))
    place = [drow // (ny * nz), (drow // nz) % ny, drow % nz]
    opposite = jnp.zeros((devices, 128), F32)
    for dy in (-1, 1):
        for dz in (-1, 1):
            mine = CORNER + 2 * (2 + (dy > 0)) + (0 if dz > 0 else 1)
            theirs = CORNER + 2 * (0 + (dy < 0)) + (1 if dz > 0 else 0)
            step = (ny + dy) * nz + dz
            ok = (place[0] < nx - 1) & (place[1] + dy >= 0) & (place[1] + dy < ny)
            ok = ok & (place[2] + dz >= 0) & (place[2] + dz < nz) & (dlane == mine)
            other = roll(roll(mom, -step, 0), mine - theirs, 1)
            opposite = opposite + jnp.where(ok, mom * other, 0.0)
    e1 = lane_of(E1) - 12.0 * total(opposite)
    r1ar1 = r1ar1 - alpha * lane_of(E0) + alpha * alpha * e1
    beta = norm1 / norm0
    alpha1 = norm1 / (r1ar1 + beta * (2.0 * r1w + beta * rw))

    xy, xz, yz = {}, {}, {}
    for dx, dy, dz in PAIRS:
        exists, at = neighbour(sizes, dx, dy, dz)
        line = pay_ref[pl.ds(2 * at + 1, 1), :] * (2.0 * exists)
        if dz == 0:
            xy[dx, dy] = line
        elif dx == 0:
            yz[dy, dz] = line
        else:
            xz[dx, dz] = jnp.sum(jnp.where(row == lane, line, 0.0), axis=1, keepdims=True)
    row8, lane8 = iotas(8)
    rim = {}
    for dy in (-1, 1):
        rim[dy] = jnp.where(lane1 % 2 == 0, roll(yz[dy, 1], -1, 1), roll(yz[dy, -1], 1, 1))
    rim = jnp.where(row8 == 0, rim[-1], jnp.where(row8 == 7, rim[1], 0.0))
    sides = (lane8 == 0) | (lane8 == 127)

    for x in range(X):
        turned = jnp.where(sides, roll(rim, -(2 * x + 1), 1), 0.0)
        for lo, hi in ((0, 8), (8, Y - 8), (Y - 8, Y)):
            sl = slice(x * Y + lo, x * Y + hi)
            r, w, s = r_ref[sl, :], w_ref[sl, :], s_ref[sl, :]
            dx = -1 if x == 0 else 1 if x == X - 1 else 0
            dy = -1 if lo == 0 else 1 if hi == Y else 0
            if dy:
                at = row8 == (0 if dy < 0 else 7)
                s = s + jnp.where(at, turned, 0.0)
                if dx:
                    s = s + jnp.where(at, xy[dx, dy], 0.0)
            if dx:
                ln = lane[lo:hi]
                s = s + jnp.where(ln == 0, xz[dx, -1][lo:hi], jnp.where(ln == 127, xz[dx, 1][lo:hi], 0.0))
            r1 = r - alpha * w
            x_out[sl, :] = alpha * r + alpha1 * (r1 + beta * r)
            r_out[sl, :] = r1 - alpha1 * (w - alpha * s + beta * w)


def per_device(face_blocks, owner_rank, owner_tile, live_count, right_side, diagonal):
    sizes = tuple(lax.axis_size(a) for a in AXES)
    nx, ny, nz = sizes
    X, Y, Z = right_side.shape
    dims = (X, Y)
    count = face_blocks.shape[3]
    side = 2 * Y
    flat = jax.ShapeDtypeStruct((X * Y, Z), F32)
    rhs, diag = right_side.reshape(X * Y, Z), diagonal.reshape(X * Y, Z)

    packed, rhs, diag = pl.pallas_call(
        functools.partial(pack_kernel, nx),
        out_shape=[jax.ShapeDtypeStruct((nx, Y + TAGS, 128), F32), flat, flat],
        in_specs=[HBM] * 6,
        out_specs=[VMEM] * 3,
        scratch_shapes=[
            pltpu.SMEM((count,), jnp.int32),
            pltpu.SMEM((count,), jnp.int32),
            pltpu.SMEM((1,), jnp.int32),
            pltpu.VMEM((count, side, side), F32),
            pltpu.SemaphoreType.DMA((3,)),
            pltpu.SemaphoreType.DMA((count,)),
            pltpu.SemaphoreType.DMA((2,)),
        ],
        compiler_params=params(),
        name="pack",
    )(
        in_hbm(owner_rank.reshape(count)),
        in_hbm(owner_tile.reshape(count)),
        live_count.reshape(1),
        in_hbm(face_blocks.reshape(count, side, side)),
        in_hbm(rhs),
        in_hbm(diag),
    )
    chunks = [packed[0]]
    for k in range(1, nx):
        chunks.append(lax.ppermute(packed[k], "gx", [(i, peer(i, k, nx)) for i in range(nx)]))

    def face_shapes():
        shapes = [(2 * Y, Z)] * len(matchings(nx)) + [(2 * X, Z)] * len(matchings(ny)) + [(Y, Z)]
        return [jax.ShapeDtypeStruct(s, F32) for s in shapes]

    r, pw, *faces = pl.pallas_call(
        functools.partial(load_kernel, sizes, dims),
        out_shape=[flat, flat] + face_shapes(),
        in_specs=[VMEM] * (nx + 2),
        out_specs=[VMEM] * (2 + len(face_shapes())),
        scratch_shapes=[pltpu.VMEM((nx * Y, 128), F32)],
        compiler_params=params(),
        name="load",
    )(*chunks, rhs, diag)
    tile = faces[-1]
    got = []
    sent = iter(faces[:-1])
    for axis, n in (("gx", nx), ("gy", ny), ("gz", nz)):
        for pairs in matchings(n):
            face = tile if axis == "gz" else next(sent)
            got.append(lax.ppermute(face, axis, pairs))

    w, s, pay = pl.pallas_call(
        functools.partial(moment_kernel, sizes, dims),
        out_shape=[flat, flat, jax.ShapeDtypeStruct((2 * nx * ny * nz, 128), F32)],
        in_specs=[VMEM] * (4 + len(got)),
        out_specs=[VMEM] * 3,
        scratch_shapes=[pltpu.VMEM((X * Y, 128), F32)],
        compiler_params=params(),
        name="moments",
    )(r, pw, diag, tile, *got)
    pay = lax.all_to_all(pay, AXES, split_axis=0, concat_axis=0, tiled=True)
    x2, r2 = pl.pallas_call(
        functools.partial(final_kernel, sizes, dims),
        out_shape=[flat, flat],
        in_specs=[VMEM] * 4,
        out_specs=[VMEM] * 2,
        compiler_params=params(),
        name="final",
    )(pay, r, w, s)
    return x2.reshape(X, Y, Z), r2.reshape(X, Y, Z)


def solution(mesh):
    return jax.shard_map(
        per_device,
        mesh=mesh,
        in_specs=(
            P("gx", "gy", "gz", None, None),
            P("gx", "gy", "gz", None, None),
            P("gx", "gy", "gz", None),
            P("gx", "gy", "gz"),
            P("gx", "gy", "gz"),
            P("gx", "gy", "gz"),
        ),
        out_specs=(P("gx", "gy", "gz"), P("gx", "gy", "gz")),
        check_vma=False,
    )
```
